32 devices in a mesh: dp: 1 (over z), tp: 32 (over x, y, core).
Axes of the slice: x: 4, y: 4, z: 1, core: 2. Of those that a mesh axis runs over, the one named last changes fastest.
The devices are a block of a 4x4x8 slice.
Arguments:
- x: bfloat16 [2048, 7168], P('dp')
- dy: bfloat16 [2048, 7168], P('dp')
- gate: bfloat16 [2048, 20480], P('dp', 'tp')
- up: bfloat16 [2048, 20480], P('dp', 'tp')
- w_gate: bfloat16 [7168, 20480], P(None, 'tp')
- w_up: bfloat16 [7168, 20480], P(None, 'tp')
- w_down: bfloat16 [20480, 7168], P('tp')
Outputs:
- output 1: bfloat16 [2048, 7168], P('dp')
- output 2: bfloat16 [7168, 20480], P('dp', 'tp')
- output 3: bfloat16 [7168, 20480], P('dp', 'tp')
- output 4: bfloat16 [20480, 7168], P(('dp', 'tp'))
All inputs are finite; a program needn't handle non-finite values.
Results may differ from the reference program's by a relative error of at most 0.012.
Values are sent between devices in bfloat16 or wider.
A program may use at most 768 MiB of HBM per device.

```python
import jax
import jax.numpy as jnp

ROWS = 2048
D = 7168
FF = 20480


def act(gate, up):
    return jax.nn.silu(gate) * up


def setup_inputs(seed: int = 0, part: int = 0) -> dict:
    kx, ky, ka, kb, kg, ku, kd = jax.random.split(jax.random.key(seed), 7)
    kx, ky, ka, kb = (jax.random.fold_in(k, part) for k in (kx, ky, ka, kb))
    drawn = {
        "x": jax.random.normal(kx, (ROWS, D), jnp.float32),
        "dy": jax.random.normal(ky, (ROWS, D), jnp.float32),
        "gate": jax.random.normal(ka, (ROWS, FF), jnp.float32),
        "up": jax.random.normal(kb, (ROWS, FF), jnp.float32),
        "w_gate": jax.random.normal(kg, (D, FF), jnp.float32) * D**-0.5,
        "w_up": jax.random.normal(ku, (D, FF), jnp.float32) * D**-0.5,
        "w_down": jax.random.normal(kd, (FF, D), jnp.float32) * FF**-0.5,
    }
    return {k: v.astype(jnp.bfloat16) for k, v in drawn.items()}


def reference(x, dy, gate, up, w_gate, w_up, w_down):
    hidden, back = jax.vjp(act, gate.astype(jnp.float32), up.astype(jnp.float32))
    d_hidden = jnp.dot(dy, w_down.T, preferred_element_type=jnp.float32)
    d_gate, d_up = (g.astype(jnp.bfloat16) for g in back(d_hidden))
    dx = jnp.dot(d_gate, w_gate.T, preferred_element_type=jnp.float32) + jnp.dot(d_up, w_up.T, preferred_element_type=jnp.float32)
    dw_gate = jnp.dot(x.T, d_gate, preferred_element_type=jnp.float32)
    dw_up = jnp.dot(x.T, d_up, preferred_element_type=jnp.float32)
    dw_down = jnp.dot(hidden.astype(jnp.bfloat16).T, dy, preferred_element_type=jnp.float32)
    return tuple(g.astype(jnp.bfloat16) for g in (dx, dw_gate, dw_up, dw_down))
```

```python
import functools

import jax
import jax.numpy as jnp
from jax import lax
from jax.experimental import pallas as pl
from jax.experimental.pallas import tpu as pltpu
from jax.sharding import PartitionSpec as P

MESH = pl.DeviceIdType.MESH
BF16, F32 = jnp.bfloat16, jnp.float32
R = 256
L = 128
SIDE = 4
GROUPS = 2
NT = (((1,), (1,)), ((), ()))
VMEM_LIMIT = 66_900_000


def reduce_kernel(
    nch, dy, gate, up, wg, wu, wd, grads, *rest
):
    outs = rest[:GROUPS]
    (w, wdv, dyv, gv, uv, dh, dt, obuf, pbuf, cs, s1a, r1a, s1b, r1b, p1, s2a, r2a, s2b, r2b, fin,
     in_sem, w_sem, dt_sem, fin_sem, ps, pr, ss1a, sr1a, ss1b, sr1b, ss2a, sr2a, ss2b, sr2b,
     cp, c1a, c1b, c2a, c2b) = rest[GROUPS:]
    f = wg.shape[1]
    half = wg.shape[0] // 2
    quarter = half // SIDE
    sub = quarter // SIDE
    hs = sub // 2
    per_group = nch // GROUPS

    me = lax.axis_index("tp")
    core = lax.rem(me, 2)
    y = lax.rem(me // 2, SIDE)
    x = me // (2 * SIDE)

    def at(i, j, c):
        return (lax.rem(i + SIDE, SIDE) * SIDE + lax.rem(j + SIDE, SIDE)) * 2 + c

    partner = at(x, y, 1 - core)
    xn = (at(x + 1, y, core), at(x - 1, y, core))
    yn = (at(x, y + 1, core), at(x, y - 1, core))
    ring1, pos1 = (xn, yn), (x, y)
    ring2, pos2 = (yn, xn), (y, x)

    def fetch(k):
        rows = pl.ds(pl.multiple_of(k * R, R), R)
        return [
            pltpu.make_async_copy(dy.at[rows], dyv, in_sem.at[0]),
            pltpu.make_async_copy(gate.at[rows], gv, in_sem.at[1]),
            pltpu.make_async_copy(up.at[rows], uv, in_sem.at[2]),
        ]

    wcopies = [
        pltpu.make_async_copy(wd, wdv, w_sem.at[0]),
        pltpu.make_async_copy(wg, w.at[:, pl.ds(0, f)], w_sem.at[1]),
        pltpu.make_async_copy(wu, w.at[:, pl.ds(f, f)], w_sem.at[2]),
    ]
    first = fetch(0)
    first[0].start()
    wcopies[0].start()
    first[1].start()
    first[2].start()
    wcopies[1].start()
    wcopies[2].start()

    barrier = pltpu.get_barrier_semaphore()
    for peer in (partner, *xn, *yn):
        pl.semaphore_signal(barrier, inc=1, device_id={"tp": peer}, device_id_type=MESH)
    pl.semaphore_wait(barrier, 5)

    def remote(src, dst, ssem, rsem, dev):
        return pltpu.make_async_remote_copy(
            src_ref=src, dst_ref=dst, send_sem=ssem, recv_sem=rsem,
            device_id={"tp": dev}, device_id_type=MESH,
        )

    def pair_copy(k, a):
        s = lax.rem(k, 2)
        return remote(obuf.at[s, a], pbuf.at[s, a], ps.at[s, a], pr.at[s, a], partner)

    def hop(k, c, d, src, dst, ssem, rsem, ring):
        s = lax.rem(k, 2)
        return remote(src.at[s, c, d], dst.at[s, c, d], ssem.at[s, c, d], rsem.at[s, c, d], ring[c][d])

    h1a = lambda k, c, d: hop(k, c, d, s1a, r1a, ss1a, sr1a, ring1)
    h1b = lambda k, c, d: hop(k, c, d, s1b, r1b, ss1b, sr1b, ring1)
    h2a = lambda k, c, d: hop(k, c, d, s2a, r2a, ss2a, sr2a, ring2)
    h2b = lambda k, c, d: hop(k, c, d, s2b, r2b, ss2b, sr2b, ring2)
    CD = [(c, d) for c in range(2) for d in range(2)]

    def before_fill(k, h):
        @pl.when(k >= 2)
        def _():
            for c, d in CD:
                h(k - 2, c, d).wait_send()

    def launch(k, h, credit):
        @pl.when(k >= 2)
        def _():
            for c, d in CD:
                pl.semaphore_wait(credit.at[c, d], 1)
        for c, d in CD:
            h(k, c, d).start()

    def give_credit(k, credit, ring):
        @pl.when(k + 2 < nch)
        def _():
            for c, d in CD:
                pl.semaphore_signal(
                    credit.at[c, d], inc=1, device_id={"tp": ring[c][1 - d]}, device_id_type=MESH
                )

    def ring_at(p, off):
        return lax.rem(p + off, SIDE)

    def piece(s, c, q):
        if c == 0:
            return lambda lo, n: cs[s, q, pl.ds(lo, n), :, pl.ds(0, L)]
        return lambda lo, n: cs[s, pl.ds(lo, n), q, :, pl.ds(L, L)]

    def grads_copy(k):
        s = lax.rem(k, 2)
        return pltpu.make_async_copy(
            dt.at[s], grads.at[:, pl.ds(pl.multiple_of(k * R, R), R)], dt_sem.at[s]
        )

    def stage_a(k):
        s = lax.rem(k, 2)
        for c in fetch(k):
            c.wait()

        @pl.when(k == 0)
        def _():
            wcopies[0].wait()

        depth = dyv.shape[1] // 4
        dh[...] = jnp.zeros_like(dh)

        @pl.loop(0, 4)
        def _(j):
            cols = pl.ds(pl.multiple_of(j * depth, depth), depth)
            dh[...] += lax.dot_general(wdv[:, cols], dyv[:, cols], NT, preferred_element_type=F32)

        @pl.when(k >= 2)
        def _():
            grads_copy(k - 2).wait()

        g = gv[...].astype(F32).T
        u = uv[...].astype(F32).T
        d = dh[...]
        sig = 1.0 / (1.0 + jnp.exp(-g))
        silu = g * sig
        dt[s, pl.ds(2 * f, f)] = (silu * u).astype(BF16)
        dt[s, pl.ds(f, f)] = (d * silu).astype(BF16)
        dt[s, pl.ds(0, f)] = (d * u * (sig + silu * (1.0 - sig))).astype(BF16)
        grads_copy(k).start()

        @pl.when(k + 1 < nch)
        def _():
            for c in fetch(k + 1):
                c.start()

    def rows_of(h, a):
        return pl.ds(pl.multiple_of(h * half + a * quarter, quarter), quarter)

    def stage_b(k):
        s = lax.rem(k, 2)

        @pl.when(k == 0)
        def _():
            wcopies[1].wait()
            wcopies[2].wait()

        @pl.when(k >= 2)
        def _():
            pl.semaphore_wait(cp, 1)

        @pl.loop(0, SIDE)
        def _(a):
            @pl.when(k >= 2)
            def _():
                pair_copy(k - 2, a).wait_send()

            t = jnp.dot(w[rows_of(1 - core, a)], dt[s, pl.ds(0, 2 * f)], preferred_element_type=F32)
            obuf[s, a] = t.astype(BF16).reshape(SIDE, sub, R)
            pair_copy(k, a).start()

    def stage_c(k):
        s = lax.rem(k, 2)

        @pl.loop(0, SIDE)
        def _(a):
            t = jnp.dot(w[rows_of(core, a)], dt[s, pl.ds(0, 2 * f)], preferred_element_type=F32)
            pair_copy(k, a).wait_recv()
            cs[s, a] = t.reshape(SIDE, sub, R) + pbuf[s, a].astype(F32)

        @pl.when(k + 2 < nch)
        def _():
            pl.semaphore_signal(cp, inc=1, device_id={"tp": partner}, device_id_type=MESH)

    def stage_1a(k):
        s = lax.rem(k, 2)
        before_fill(k, h1a)
        for c in range(2):
            take = piece(s, c, ring_at(pos1[c], 2))
            for d in range(2):
                s1a[s, c, d] = take(2 * d, 2).astype(BF16)
        launch(k, h1a, c1a)

    def stage_1b(k):
        s = lax.rem(k, 2)
        before_fill(k, h1b)
        for c, d in CD:
            h1a(k, c, d).wait_recv()
            take = piece(s, c, ring_at(pos1[c], 1 if d == 0 else SIDE - 1))
            s1b[s, c, d, pl.ds(2 * d, 2)] = (take(2 * d, 2) + r1a[s, c, d].astype(F32)).astype(BF16)
            s1b[s, c, d, pl.ds(2 - 2 * d, 2)] = take(2 - 2 * d, 2).astype(BF16)
        launch(k, h1b, c1b)
        give_credit(k, c1a, ring1)

    def stage_1c(k):
        s = lax.rem(k, 2)
        for c in range(2):
            for d in range(2):
                h1b(k, c, d).wait_recv()
            p1[s, c] = piece(s, c, pos1[c])(0, SIDE) + r1b[s, c, 0].astype(F32) + r1b[s, c, 1].astype(F32)
        give_credit(k, c1b, ring1)

    def stage_2a(k):
        s = lax.rem(k, 2)
        before_fill(k, h2a)
        for c, d in CD:
            s2a[s, c, d] = p1[s, c, ring_at(pos2[c], 2), pl.ds(d * hs, hs)].astype(BF16)
        launch(k, h2a, c2a)

    def stage_2b(k):
        s = lax.rem(k, 2)
        before_fill(k, h2b)
        for c, d in CD:
            h2a(k, c, d).wait_recv()
            q = ring_at(pos2[c], 1 if d == 0 else SIDE - 1)
            same, other = pl.ds(d * hs, hs), pl.ds((1 - d) * hs, hs)
            s2b[s, c, d, same] = (p1[s, c, q, same] + r2a[s, c, d].astype(F32)).astype(BF16)
            s2b[s, c, d, other] = p1[s, c, q, other].astype(BF16)
        launch(k, h2b, c2b)
        give_credit(k, c2a, ring2)

    def fin_copies(k):
        s = lax.rem(k, 2)
        return [
            (g, pltpu.make_async_copy(fin.at[s], o.at[k - g * per_group], fin_sem.at[s]))
            for g, o in enumerate(outs)
        ]

    def of_group(k, act):
        for g, copy in fin_copies(k):
            @pl.when((k >= g * per_group) & (k < (g + 1) * per_group))
            def _():
                act(copy)

    def stage_2c(k):
        s = lax.rem(k, 2)

        @pl.when(k >= 2)
        def _():
            of_group(k - 2, lambda copy: copy.wait())

        for c in range(2):
            for d in range(2):
                h2b(k, c, d).wait_recv()
            total = p1[s, c, pos2[c]] + r2b[s, c, 0].astype(F32) + r2b[s, c, 1].astype(F32)
            fin[s, c] = total.astype(BF16)
        of_group(k, lambda copy: copy.start())
        give_credit(k, c2b, ring2)

    def run(stage, k):
        @pl.when((k >= 0) & (k < nch))
        def _():
            stage(k)

    @pl.loop(0, nch + 4)
    def _(i):
        run(stage_a, i)
        run(stage_2b, i - 4)
        run(stage_b, i)
        run(stage_1c, i - 3)
        run(stage_2a, i - 3)
        run(stage_1b, i - 2)
        run(stage_c, i - 1)
        run(stage_1a, i - 1)
        run(stage_2c, i - 4)

    for k in (nch - 2, nch - 1):
        grads_copy(k).wait()
        for a in range(SIDE):
            pair_copy(k, a).wait_send()
        for h in (h1a, h1b, h2a, h2b):
            for c, d in CD:
                h(k, c, d).wait_send()
        g = k // per_group
        pltpu.make_async_copy(fin.at[k % 2], outs[g].at[k - g * per_group], fin_sem.at[k % 2]).wait()


def reduce_call(dy, gate, up, wg, wu, wd):
    rows, d = dy.shape
    f = wg.shape[1]
    nch = rows // R
    sub = d // (2 * SIDE * SIDE)
    quarter = sub * SIDE
    ANY = pl.BlockSpec(memory_space=pl.ANY)
    dma = pltpu.SemaphoreType.DMA
    return pl.pallas_call(
        functools.partial(reduce_kernel, nch),
        out_shape=[jax.ShapeDtypeStruct((3 * f, rows), BF16)]
        + [jax.ShapeDtypeStruct((nch // GROUPS, 2, sub, L), BF16)] * GROUPS,
        in_specs=[ANY] * 6,
        out_specs=[ANY] * (1 + GROUPS),
        scratch_shapes=[
            pltpu.VMEM((d, 2 * f), BF16),
            pltpu.VMEM((f, d), BF16),
            pltpu.VMEM((R, d), BF16),
            pltpu.VMEM((R, f), BF16),
            pltpu.VMEM((R, f), BF16),
            pltpu.VMEM((f, R), F32),
            pltpu.VMEM((2, 3 * f, R), BF16),
            pltpu.VMEM((2, SIDE, SIDE, sub, R), BF16),
            pltpu.VMEM((2, SIDE, SIDE, sub, R), BF16),
            pltpu.VMEM((2, SIDE, SIDE, sub, R), F32),
            pltpu.VMEM((2, 2, 2, 2, sub, L), BF16),
            pltpu.VMEM((2, 2, 2, 2, sub, L), BF16),
            pltpu.VMEM((2, 2, 2, SIDE, sub, L), BF16),
            pltpu.VMEM((2, 2, 2, SIDE, sub, L), BF16),
            pltpu.VMEM((2, 2, SIDE, sub, L), F32),
            pltpu.VMEM((2, 2, 2, sub // 2, L), BF16),
            pltpu.VMEM((2, 2, 2, sub // 2, L), BF16),
            pltpu.VMEM((2, 2, 2, sub, L), BF16),
            pltpu.VMEM((2, 2, 2, sub, L), BF16),
            pltpu.VMEM((2, 2, sub, L), BF16),
            dma((3,)),
            dma((3,)),
            dma((2,)),
            dma((2,)),
            dma((2, SIDE)),
            dma((2, SIDE)),
        ]
        + [dma((2, 2, 2))] * 8
        + [pltpu.SemaphoreType.REGULAR]
        + [pltpu.SemaphoreType.REGULAR((2, 2))] * 4,
        compiler_params=pltpu.CompilerParams(
            collective_id=0, has_side_effects=True, vmem_limit_bytes=VMEM_LIMIT
        ),
        cost_estimate=pl.CostEstimate(
            flops=6 * rows * d * f, bytes_accessed=2 * (rows * d + 3 * d * f), transcendentals=rows * f
        ),
        name="terms_reduce_scatter",
    )(dy, gate, up, wg, wu, wd)


def weights_kernel(x, dy, grads, dwg, dwu, dwd, done):
    f = dwd.shape[0]
    done[...] = jnp.zeros_like(done)
    for i, out in enumerate((dwg, dwu)):
        t = jnp.dot(grads[pl.ds(i * f, f)], x[...], preferred_element_type=F32)
        out[...] = t.T.astype(BF16)
    dwd[...] = jnp.dot(grads[pl.ds(2 * f, f)], dy[...], preferred_element_type=F32).astype(BF16)


def weights_call(x, dy, grads):
    rows, d = x.shape
    f = grads.shape[0] // 3
    n = min(512, d)
    return pl.pallas_call(
        weights_kernel,
        grid=(d // n,),
        out_shape=[
            jax.ShapeDtypeStruct((d, f), BF16),
            jax.ShapeDtypeStruct((d, f), BF16),
            jax.ShapeDtypeStruct((f, d), BF16),
            jax.ShapeDtypeStruct((8, 128), F32),
        ],
        in_specs=[
            pl.BlockSpec((rows, n), lambda j: (0, j)),
            pl.BlockSpec((rows, n), lambda j: (0, j)),
            pl.BlockSpec((3 * f, rows), lambda j: (0, 0), pipeline_mode=pl.Buffered(1)),
        ],
        out_specs=[
            pl.BlockSpec((n, f), lambda j: (j, 0)),
            pl.BlockSpec((n, f), lambda j: (j, 0)),
            pl.BlockSpec((f, n), lambda j: (0, j)),
            pl.BlockSpec((8, 128), lambda j: (0, 0)),
        ],
        compiler_params=pltpu.CompilerParams(vmem_limit_bytes=56 * 2**20),
        cost_estimate=pl.CostEstimate(
            flops=6 * rows * d * f, bytes_accessed=2 * (2 * rows * d + 3 * d * f), transcendentals=0
        ),
        name="weight_gradients",
    )(x, dy, grads)


def place_kernel(g, *refs):
    out = refs[-1]
    for c in range(2):
        stacked = jnp.concatenate([g[0, b, 0, 0, c] for b in range(SIDE)], axis=0)
        out[0, pl.ds(c * L, L)] = stacked.T


def place_call(g, gathered, into, nch, after):
    n, per_group, _, sub, _ = gathered.shape
    quarter = sub * SIDE
    d = quarter * SIDE * 2
    view = gathered.reshape(SIDE, SIDE, 2, per_group, 2, sub, L)
    ANY = pl.BlockSpec(memory_space=pl.ANY)
    extra = [into] if into is not None else []
    return pl.pallas_call(
        place_kernel,
        grid=(per_group, 2, SIDE),
        out_shape=jax.ShapeDtypeStruct((nch, R, d), BF16),
        in_specs=[
            pl.BlockSpec((1, SIDE, 1, 1, 2, sub, L), lambda k, c, a: (a, 0, c, k, 0, 0, 0)),
            ANY,
        ] + [ANY] * len(extra),
        out_specs=pl.BlockSpec((1, R, quarter), lambda k, c, a: (g * per_group + k, 0, c * SIDE + a)),
        input_output_aliases={2: 0} if extra else {},
        compiler_params=pltpu.CompilerParams(vmem_limit_bytes=32 * 2**20),
        cost_estimate=pl.CostEstimate(flops=n * per_group * sub * L * 200, bytes_accessed=8 * n * per_group * sub * L, transcendentals=0),
        name="place",
    )(view, after, *extra)


def solution(mesh):
    def step(x, dy, gate, up, w_gate, w_up, w_down):
        rows, d = x.shape
        nch = rows // R
        grads, *parts = reduce_call(dy, gate, up, w_gate, w_up, w_down)
        whole = [lax.all_gather(p, "tp", axis=0) for p in parts]
        dw_gate, dw_up, dw_down, done = weights_call(x, dy, grads)
        dx = None
        for g, part in enumerate(whole):
            dx = place_call(g, part, dx, nch, done)
        return dx.reshape(rows, d), dw_gate, dw_up, dw_down

    tokens, columns, rows = P("dp", None), P(None, "tp"), P("tp", None)
    return jax.shard_map(
        step,
        mesh=mesh,
        in_specs=(tokens, tokens, P("dp", "tp"), P("dp", "tp"), columns, columns, rows),
        out_specs=(tokens, P("dp", "tp"), P("dp", "tp"), P(("dp", "tp"), None)),
        check_vma=False,
    )
```

```python
import functools

import jax
import jax.numpy as jnp
from jax import lax
from jax.experimental import pallas as pl
from jax.experimental.pallas import tpu as pltpu
from jax.sharding import PartitionSpec as P

MESH = pl.DeviceIdType.MESH
BF16, F32 = jnp.bfloat16, jnp.float32
R = 256
L = 128
SIDE = 4
N = 256
O3A, O3B, O4A, O4B, O5 = 4, 5, 6, 8, 9
NT = (((1,), (1,)), ((), ()))
VMEM_LIMIT = 66_900_000


def block_kernel(
    nch, x_in, dy, gate, up, wg, wu, wd, grads, whole, dwg, dwu, dwd,
    dyv, gv, uv, dh, dt, obuf, pbuf, cs, s1a, r1a, s1b, r1b, p1, s2a, r2a, s2b, r2b, fin,
    in_sem, w_sem, dt_sem, fin_sem, ps, pr, ss1a, sr1a, ss1b, sr1b, ss2a, sr2a, ss2b, sr2b,
    ss3a, sr3a, ss3b, sr3b, ss4a, sr4a, ss4b, sr4b, ss5, sr5, g_sem, x_sem, o_sem,
    cp, c1a, c1b, c2a, c2b,
):
    f = wg.shape[1]
    half = wg.shape[0] // 2
    quarter = half // SIDE
    sub = quarter // SIDE
    hs = sub // 2

    me = lax.axis_index("tp")
    core = lax.rem(me, 2)
    y = lax.rem(me // 2, SIDE)
    x = me // (2 * SIDE)

    def at(i, j, c):
        return (lax.rem(i + SIDE, SIDE) * SIDE + lax.rem(j + SIDE, SIDE)) * 2 + c

    partner = at(x, y, 1 - core)
    xn = (at(x + 1, y, core), at(x - 1, y, core))
    yn = (at(x, y + 1, core), at(x, y - 1, core))
    ring1, pos1 = (xn, yn), (x, y)
    ring2, pos2 = (yn, xn), (y, x)

    def fetch(k):
        rows = pl.ds(pl.multiple_of(k * R, R), R)
        return [
            pltpu.make_async_copy(dy.at[rows], dyv, in_sem.at[0]),
            pltpu.make_async_copy(gate.at[rows], gv, in_sem.at[1]),
            pltpu.make_async_copy(up.at[rows], uv, in_sem.at[2]),
        ]

    def weight_copies(w, wdv):
        return [
            pltpu.make_async_copy(wd, wdv, w_sem.at[0]),
            pltpu.make_async_copy(wg, w.at[:, pl.ds(0, f)], w_sem.at[1]),
            pltpu.make_async_copy(wu, w.at[:, pl.ds(f, f)], w_sem.at[2]),
        ]

    def remote(src, dst, ssem, rsem, dev):
        return pltpu.make_async_remote_copy(
            src_ref=src, dst_ref=dst, send_sem=ssem, recv_sem=rsem,
            device_id={"tp": dev}, device_id_type=MESH,
        )

    def pair_copy(k, a):
        s = lax.rem(k, 2)
        return remote(obuf.at[s, a], pbuf.at[s, a], ps.at[s, a], pr.at[s, a], partner)

    def hop(k, c, d, src, dst, ssem, rsem, ring):
        s = lax.rem(k, 2)
        return remote(src.at[s, c, d], dst.at[s, c, d], ssem.at[s, c, d], rsem.at[s, c, d], ring[c][d])

    h1a = lambda k, c, d: hop(k, c, d, s1a, r1a, ss1a, sr1a, ring1)
    h1b = lambda k, c, d: hop(k, c, d, s1b, r1b, ss1b, sr1b, ring1)
    h2a = lambda k, c, d: hop(k, c, d, s2a, r2a, ss2a, sr2a, ring2)
    h2b = lambda k, c, d: hop(k, c, d, s2b, r2b, ss2b, sr2b, ring2)
    CD = [(c, d) for c in range(2) for d in range(2)]

    def before_fill(k, h):
        @pl.when(k >= 2)
        def _():
            for c, d in CD:
                h(k - 2, c, d).wait_send()

    def launch(k, h, credit):
        @pl.when(k >= 2)
        def _():
            for c, d in CD:
                pl.semaphore_wait(credit.at[c, d], 1)
        for c, d in CD:
            h(k, c, d).start()

    def give_credit(k, credit, ring):
        @pl.when(k + 2 < nch)
        def _():
            for c, d in CD:
                pl.semaphore_signal(
                    credit.at[c, d], inc=1, device_id={"tp": ring[c][1 - d]}, device_id_type=MESH
                )

    def ring_at(p, off):
        return lax.rem(p + off, SIDE)

    def piece(s, c, q):
        if c == 0:
            return lambda lo, n: cs[s, q, pl.ds(lo, n), :, pl.ds(0, L)]
        return lambda lo, n: cs[s, pl.ds(lo, n), q, :, pl.ds(L, L)]

    def grads_copy(k):
        s = lax.rem(k, 2)
        return pltpu.make_async_copy(
            dt.at[s], grads.at[:, pl.ds(pl.multiple_of(k * R, R), R)], dt_sem.at[s]
        )

    def stage_a(w, wdv, k):
        s = lax.rem(k, 2)
        for c in fetch(k):
            c.wait()

        @pl.when(k == 0)
        def _():
            weight_copies(w, wdv)[0].wait()

        depth = dyv.shape[1] // 4
        dh[...] = jnp.zeros_like(dh)

        @pl.loop(0, 4)
        def _(j):
            cols = pl.ds(pl.multiple_of(j * depth, depth), depth)
            dh[...] += lax.dot_general(wdv[:, cols], dyv[:, cols], NT, preferred_element_type=F32)

        @pl.when(k >= 2)
        def _():
            grads_copy(k - 2).wait()

        g = gv[...].astype(F32).T
        u = uv[...].astype(F32).T
        d = dh[...]
        sig = 1.0 / (1.0 + jnp.exp(-g))
        silu = g * sig
        dt[s, pl.ds(2 * f, f)] = (silu * u).astype(BF16)
        dt[s, pl.ds(f, f)] = (d * silu).astype(BF16)
        dt[s, pl.ds(0, f)] = (d * u * (sig + silu * (1.0 - sig))).astype(BF16)
        grads_copy(k).start()

        @pl.when(k + 1 < nch)
        def _():
            for c in fetch(k + 1):
                c.start()

    def rows_of(h, a):
        return pl.ds(pl.multiple_of(h * half + a * quarter, quarter), quarter)

    def stage_b(w, wdv, k):
        s = lax.rem(k, 2)

        @pl.when(k == 0)
        def _():
            for copy in weight_copies(w, wdv)[1:]:
                copy.wait()

        @pl.when(k >= 2)
        def _():
            pl.semaphore_wait(cp, 1)

        @pl.loop(0, SIDE)
        def _(a):
            @pl.when(k >= 2)
            def _():
                pair_copy(k - 2, a).wait_send()

            t = jnp.dot(w[rows_of(1 - core, a)], dt[s, pl.ds(0, 2 * f)], preferred_element_type=F32)
            obuf[s, a] = t.astype(BF16).reshape(SIDE, sub, R)
            pair_copy(k, a).start()

    def stage_c(w, wdv, k):
        s = lax.rem(k, 2)

        @pl.loop(0, SIDE)
        def _(a):
            t = jnp.dot(w[rows_of(core, a)], dt[s, pl.ds(0, 2 * f)], preferred_element_type=F32)
            pair_copy(k, a).wait_recv()
            cs[s, a] = t.reshape(SIDE, sub, R) + pbuf[s, a].astype(F32)

        @pl.when(k + 2 < nch)
        def _():
            pl.semaphore_signal(cp, inc=1, device_id={"tp": partner}, device_id_type=MESH)

    def stage_1a(k):
        s = lax.rem(k, 2)
        before_fill(k, h1a)
        for c in range(2):
            take = piece(s, c, ring_at(pos1[c], 2))
            for d in range(2):
                s1a[s, c, d] = take(2 * d, 2).astype(BF16)
        launch(k, h1a, c1a)

    def stage_1b(k):
        s = lax.rem(k, 2)
        before_fill(k, h1b)
        for c, d in CD:
            h1a(k, c, d).wait_recv()
            take = piece(s, c, ring_at(pos1[c], 1 if d == 0 else SIDE - 1))
            s1b[s, c, d, pl.ds(2 * d, 2)] = (take(2 * d, 2) + r1a[s, c, d].astype(F32)).astype(BF16)
            s1b[s, c, d, pl.ds(2 - 2 * d, 2)] = take(2 - 2 * d, 2).astype(BF16)
        launch(k, h1b, c1b)
        give_credit(k, c1a, ring1)

    def stage_1c(k):
        s = lax.rem(k, 2)
        for c in range(2):
            for d in range(2):
                h1b(k, c, d).wait_recv()
            p1[s, c] = piece(s, c, pos1[c])(0, SIDE) + r1b[s, c, 0].astype(F32) + r1b[s, c, 1].astype(F32)
        give_credit(k, c1b, ring1)

    def stage_2a(k):
        s = lax.rem(k, 2)
        before_fill(k, h2a)
        for c, d in CD:
            s2a[s, c, d] = p1[s, c, ring_at(pos2[c], 2), pl.ds(d * hs, hs)].astype(BF16)
        launch(k, h2a, c2a)

    def stage_2b(k):
        s = lax.rem(k, 2)
        before_fill(k, h2b)
        for c, d in CD:
            h2a(k, c, d).wait_recv()
            q = ring_at(pos2[c], 1 if d == 0 else SIDE - 1)
            same, other = pl.ds(d * hs, hs), pl.ds((1 - d) * hs, hs)
            s2b[s, c, d, same] = (p1[s, c, q, same] + r2a[s, c, d].astype(F32)).astype(BF16)
            s2b[s, c, d, other] = p1[s, c, q, other].astype(BF16)
        launch(k, h2b, c2b)
        give_credit(k, c2a, ring2)

    def stage_2c(k):
        s = lax.rem(k, 2)
        for c in range(2):
            for d in range(2):
                h2b(k, c, d).wait_recv()
            total = p1[s, c, pos2[c]] + r2b[s, c, 0].astype(F32) + r2b[s, c, 1].astype(F32)
            fin[k, c] = total.astype(BF16)
        give_credit(k, c2b, ring2)

    def own_copy(k, c):
        return pltpu.make_async_copy(fin.at[k, c], whole.at[k, core, c, pos1[c], pos2[c]], fin_sem.at[k, c])

    def spread(k, c, d, src, dst, ssem, rsem, ring):
        return remote(src, dst, ssem.at[k, c, d], rsem.at[k, c, d], ring[c][d])

    def came_from(p, d):
        return ring_at(p, SIDE - 1 if d == 0 else 1)

    def h3a(k, c, d):
        dst = whole.at[k, core, c, pos1[c], pos2[c]]
        return spread(k, c, d, fin.at[k, c], dst, ss3a, sr3a, ring2)

    def h3b(k, c, d):
        at3 = whole.at[k, core, c, pos1[c], came_from(pos2[c], d), pl.ds(d * hs, hs)]
        return spread(k, c, d, at3, at3, ss3b, sr3b, ring2)

    def h4a(k, c, d):
        at4 = whole.at[k, core, c, pos1[c]]
        return spread(k, c, d, at4, at4, ss4a, sr4a, ring1)

    def h4b(k, c, d):
        at4 = whole.at[k, core, c, came_from(pos1[c], d), pl.ds(2 * d, 2)]
        return spread(k, c, d, at4, at4, ss4b, sr4b, ring1)

    def h5(k, c):
        at5 = whole.at[k, core, c]
        return remote(at5, at5, ss5.at[k, c], sr5.at[k, c], partner)

    def stage_3a(k):
        for c in range(2):
            own_copy(k, c).start()
        for c, d in CD:
            h3a(k, c, d).start()

    def stage_3b(k):
        for c, d in CD:
            h3a(k, c, d).wait_recv()
            h3b(k, c, d).start()

    def stage_4a(k):
        for c in range(2):
            own_copy(k, c).wait()
            for d in range(2):
                h3b(k, c, d).wait_recv()
            for d in range(2):
                h4a(k, c, d).start()

    def stage_4b(k):
        for c, d in CD:
            h4a(k, c, d).wait_recv()
            h4b(k, c, d).start()

    def stage_5(k):
        for c in range(2):
            for d in range(2):
                h4b(k, c, d).wait_recv()
            h5(k, c).start()

    def run(stage, k):
        @pl.when((k >= 0) & (k < nch))
        def _():
            stage(k)

    def terms(w, wdv):
        copies = weight_copies(w, wdv)
        first = fetch(0)
        first[0].start()
        copies[0].start()
        first[1].start()
        first[2].start()
        copies[1].start()
        copies[2].start()

        barrier = pltpu.get_barrier_semaphore()
        for peer in (partner, *xn, *yn):
            pl.semaphore_signal(barrier, inc=1, device_id={"tp": peer}, device_id_type=MESH)
        pl.semaphore_wait(barrier, 5)

        @pl.loop(0, nch + 1)
        def _(i):
            run(functools.partial(stage_a, w, wdv), i)
            run(stage_2b, i - 4)
            run(functools.partial(stage_b, w, wdv), i)
            run(stage_1c, i - 3)
            run(stage_2a, i - 3)
            run(stage_1b, i - 2)
            run(functools.partial(stage_c, w, wdv), i - 1)
            run(stage_1a, i - 1)
            run(stage_2c, i - 4)
            run(stage_3a, i - O3A)
            run(stage_3b, i - O3B)
            run(stage_4a, i - O4A)
            run(stage_4b, i - O4B)
            run(stage_5, i - O5)

    pl.run_scoped(terms, pltpu.VMEM((2 * half, 2 * f), BF16), pltpu.VMEM((f, 2 * half), BF16))

    for k in (nch - 2, nch - 1):
        grads_copy(k).wait()

    blocks = 2 * half // N
    tail = nch + O5
    per_step = -(-blocks // (tail - nch - 1))

    def weights(gr, xv, dv, gst, dst):
        load = pltpu.make_async_copy(grads, gr, g_sem)

        def cols(j):
            return pl.ds(pl.multiple_of(j * N, N), N)

        def ins(j):
            s = lax.rem(j, 2)
            return [
                pltpu.make_async_copy(x_in.at[:, cols(j)], xv.at[s], x_sem.at[s, 0]),
                pltpu.make_async_copy(dy.at[:, cols(j)], dv.at[s], x_sem.at[s, 1]),
            ]

        def results(j):
            s = lax.rem(j, 2)
            return [
                pltpu.make_async_copy(gst.at[s, 0], dwg.at[cols(j)], o_sem.at[s, 0]),
                pltpu.make_async_copy(gst.at[s, 1], dwu.at[cols(j)], o_sem.at[s, 1]),
                pltpu.make_async_copy(dst.at[s], dwd.at[:, cols(j)], o_sem.at[s, 2]),
            ]

        def unit(j):
            s = lax.rem(j, 2)

            @pl.when(j == 0)
            def _():
                load.wait()

            for copy in ins(j):
                copy.wait()

            @pl.when(j >= 2)
            def _():
                for copy in results(j - 2):
                    copy.wait()

            for m in range(2):
                t = jnp.dot(gr[pl.ds(m * f, f)], xv[s], preferred_element_type=F32)
                gst[s, m] = t.T.astype(BF16)
            dst[s] = jnp.dot(gr[pl.ds(2 * f, f)], dv[s], preferred_element_type=F32).astype(BF16)
            for copy in results(j):
                copy.start()

            @pl.when(j + 2 < blocks)
            def _():
                for copy in ins(j + 2):
                    copy.start()

        def units(lo, hi):
            @pl.loop(lo, hi)
            def _(j):
                @pl.when(j < blocks)
                def _():
                    unit(j)

        load.start()
        for j in (0, 1):
            for copy in ins(j):
                copy.start()

        split = per_step // 2

        @pl.loop(nch + 1, tail)
        def _(i):
            j = (i - nch - 1) * per_step
            run(stage_2b, i - 4)
            run(stage_1c, i - 3)
            run(stage_2a, i - 3)
            run(stage_1b, i - 2)
            units(j, j + split)
            run(stage_2c, i - 4)
            run(stage_3a, i - O3A)
            run(stage_3b, i - O3B)
            units(j + split, j + per_step)
            run(stage_4a, i - O4A)
            run(stage_4b, i - O4B)
            run(stage_5, i - O5)

        for j in (blocks - 2, blocks - 1):
            for copy in results(j):
                copy.wait()

    pl.run_scoped(
        weights,
        pltpu.VMEM((3 * f, nch * R), BF16),
        pltpu.VMEM((2, nch * R, N), BF16),
        pltpu.VMEM((2, nch * R, N), BF16),
        pltpu.VMEM((2, 2, N, f), BF16),
        pltpu.VMEM((2, f, N), BF16),
    )

    for k in (nch - 2, nch - 1):
        for a in range(SIDE):
            pair_copy(k, a).wait_send()
        for h in (h1a, h1b, h2a, h2b):
            for c, d in CD:
                h(k, c, d).wait_send()

    @pl.loop(0, nch)
    def _(k):
        for h in (h3a, h3b, h4a, h4b):
            for c, d in CD:
                h(k, c, d).wait_send()
        for c in range(2):
            h5(k, c).wait()


def block_call(x, dy, gate, up, wg, wu, wd):
    rows, d = dy.shape
    f = wg.shape[1]
    nch = rows // R
    sub = d // (2 * SIDE * SIDE)
    ANY = pl.BlockSpec(memory_space=pl.ANY)
    dma = pltpu.SemaphoreType.DMA
    return pl.pallas_call(
        functools.partial(block_kernel, nch),
        out_shape=[
            jax.ShapeDtypeStruct((3 * f, rows), BF16),
            jax.ShapeDtypeStruct((nch, 2, 2, SIDE, SIDE, sub, L), BF16),
            jax.ShapeDtypeStruct((d, f), BF16),
            jax.ShapeDtypeStruct((d, f), BF16),
            jax.ShapeDtypeStruct((f, d), BF16),
        ],
        in_specs=[ANY] * 7,
        out_specs=[ANY] * 5,
        scratch_shapes=[
            pltpu.VMEM((R, d), BF16),
            pltpu.VMEM((R, f), BF16),
            pltpu.VMEM((R, f), BF16),
            pltpu.VMEM((f, R), F32),
            pltpu.VMEM((2, 3 * f, R), BF16),
            pltpu.VMEM((2, SIDE, SIDE, sub, R), BF16),
            pltpu.VMEM((2, SIDE, SIDE, sub, R), BF16),
            pltpu.VMEM((2, SIDE, SIDE, sub, R), F32),
            pltpu.VMEM((2, 2, 2, 2, sub, L), BF16),
            pltpu.VMEM((2, 2, 2, 2, sub, L), BF16),
            pltpu.VMEM((2, 2, 2, SIDE, sub, L), BF16),
            pltpu.VMEM((2, 2, 2, SIDE, sub, L), BF16),
            pltpu.VMEM((2, 2, SIDE, sub, L), F32),
            pltpu.VMEM((2, 2, 2, sub // 2, L), BF16),
            pltpu.VMEM((2, 2, 2, sub // 2, L), BF16),
            pltpu.VMEM((2, 2, 2, sub, L), BF16),
            pltpu.VMEM((2, 2, 2, sub, L), BF16),
            pltpu.VMEM((nch, 2, sub, L), BF16),
            dma((3,)),
            dma((3,)),
            dma((2,)),
            dma((nch, 2)),
            dma((2, SIDE)),
            dma((2, SIDE)),
        ]
        + [dma((2, 2, 2))] * 8
        + [dma((nch, 2, 2))] * 8
        + [dma((nch, 2))] * 2
        + [dma, dma((2, 2)), dma((2, 3))]
        + [pltpu.SemaphoreType.REGULAR]
        + [pltpu.SemaphoreType.REGULAR((2, 2))] * 4,
        compiler_params=pltpu.CompilerParams(
            collective_id=0, has_side_effects=True, vmem_limit_bytes=VMEM_LIMIT
        ),
        cost_estimate=pl.CostEstimate(
            flops=12 * rows * d * f, bytes_accessed=8 * rows * d + 12 * d * f, transcendentals=rows * f
        ),
        name="mlp_backward",
    )(x, dy, gate, up, wg, wu, wd)


def place_kernel(g, out):
    for c in range(2):
        for a in range(SIDE):
            pieces = [g[0, 0, c, a, b] if c == 0 else g[0, 0, c, b, a] for b in range(SIDE)]
            stacked = jnp.concatenate(pieces, axis=0)
            n = stacked.shape[0]
            out[0, pl.ds(c * L, L), pl.ds(a * n, n)] = stacked.T


def place_call(whole):
    nch, _, _, _, _, sub, _ = whole.shape
    half = sub * SIDE * SIDE
    return pl.pallas_call(
        place_kernel,
        grid=(nch, 2),
        out_shape=jax.ShapeDtypeStruct((nch, R, 2 * half), BF16),
        in_specs=[pl.BlockSpec((1, 1, 2, SIDE, SIDE, sub, L), lambda k, c: (k, c, 0, 0, 0, 0, 0))],
        out_specs=pl.BlockSpec((1, R, half), lambda k, c: (k, 0, c)),
        compiler_params=pltpu.CompilerParams(vmem_limit_bytes=60 * 2**20),
        cost_estimate=pl.CostEstimate(
            flops=nch * R * half * 64, bytes_accessed=8 * nch * R * half, transcendentals=0
        ),
        name="place",
    )(whole)


def solution(mesh):
    def step(x, dy, gate, up, w_gate, w_up, w_down):
        _, whole, dw_gate, dw_up, dw_down = block_call(x, dy, gate, up, w_gate, w_up, w_down)
        return place_call(whole).reshape(x.shape), dw_gate, dw_up, dw_down

    tokens, columns, rows = P("dp", None), P(None, "tp"), P("tp", None)
    return jax.shard_map(
        step,
        mesh=mesh,
        in_specs=(tokens, tokens, P("dp", "tp"), P("dp", "tp"), columns, columns, rows),
        out_specs=(tokens, P("dp", "tp"), P("dp", "tp"), P(("dp", "tp"), None)),
        check_vma=False,
    )
```

```python
import functools

import jax
import jax.numpy as jnp
from jax import lax
from jax.experimental import pallas as pl
from jax.experimental.pallas import tpu as pltpu
from jax.sharding import PartitionSpec as P

MESH = pl.DeviceIdType.MESH
BF16, F32 = jnp.bfloat16, jnp.float32
R = 256
L = 128
SIDE = 4
N = 256
O3A, O3B, O4A, O4B, O5 = 6, 7, 8, 9, 10
NT = (((1,), (1,)), ((), ()))
VMEM_LIMIT = 66_900_000


def block_kernel(
    nch, x_in, dy, gate, up, wg, wu, wd, grads, whole, dwg, dwu, dwd,
    dyv, gv, uv, dh, dt, obuf, pbuf, cs, s1a, r1a, s1b, r1b, p1, s2a, r2a, s2b, r2b, fin,
    in_sem, w_sem, dt_sem, fin_sem, ps, pr, ss1a, sr1a, ss1b, sr1b, ss2a, sr2a, ss2b, sr2b,
    ss3a, sr3a, ss3b, sr3b, ss4a, sr4a, ss4b, sr4b, ss5, sr5, g_sem, x_sem, o_sem,
    cp, c1a, c1b, c2a, c2b,
):
    f = wg.shape[1]
    half = wg.shape[0] // 2
    quarter = half // SIDE
    sub = quarter // SIDE
    hs = sub // 2

    me = lax.axis_index("tp")
    core = lax.rem(me, 2)
    y = lax.rem(me // 2, SIDE)
    x = me // (2 * SIDE)

    def at(i, j, c):
        return (lax.rem(i + SIDE, SIDE) * SIDE + lax.rem(j + SIDE, SIDE)) * 2 + c

    partner = at(x, y, 1 - core)
    xn = (at(x + 1, y, core), at(x - 1, y, core))
    yn = (at(x, y + 1, core), at(x, y - 1, core))
    ring1, pos1 = (xn, yn), (x, y)
    ring2, pos2 = (yn, xn), (y, x)

    def fetch(k):
        rows = pl.ds(pl.multiple_of(k * R, R), R)
        return [
            pltpu.make_async_copy(dy.at[rows], dyv, in_sem.at[0]),
            pltpu.make_async_copy(gate.at[rows], gv, in_sem.at[1]),
            pltpu.make_async_copy(up.at[rows], uv, in_sem.at[2]),
        ]

    def weight_copies(w, wdv):
        copies = [pltpu.make_async_copy(wd, wdv, w_sem.at[0])]
        for i, h in enumerate((1 - core, core)):
            rows = pl.ds(pl.multiple_of(h * half, half), half)
            for m, source in enumerate((wg, wu)):
                copies.append(
                    pltpu.make_async_copy(
                        source.at[rows], w.at[rows, pl.ds(m * f, f)], w_sem.at[1 + 2 * i + m]
                    )
                )
        return copies

    def remote(src, dst, ssem, rsem, dev):
        return pltpu.make_async_remote_copy(
            src_ref=src, dst_ref=dst, send_sem=ssem, recv_sem=rsem,
            device_id={"tp": dev}, device_id_type=MESH,
        )

    def pair_copy(k, a):
        s = lax.rem(k, 2)
        return remote(obuf.at[s, a], pbuf.at[s, a], ps.at[s, a], pr.at[s, a], partner)

    def hop(k, c, d, src, dst, ssem, rsem, ring):
        s = lax.rem(k, 2)
        return remote(src.at[s, c, d], dst.at[s, c, d], ssem.at[s, c, d], rsem.at[s, c, d], ring[c][d])

    h1a = lambda k, c, d: hop(k, c, d, s1a, r1a, ss1a, sr1a, ring1)
    h1b = lambda k, c, d: hop(k, c, d, s1b, r1b, ss1b, sr1b, ring1)
    h2a = lambda k, c, d: hop(k, c, d, s2a, r2a, ss2a, sr2a, ring2)
    h2b = lambda k, c, d: hop(k, c, d, s2b, r2b, ss2b, sr2b, ring2)
    CD = [(c, d) for c in range(2) for d in range(2)]

    def before_fill(k, h):
        @pl.when(k >= 2)
        def _():
            for c, d in CD:
                h(k - 2, c, d).wait_send()

    def launch(k, h, credit):
        @pl.when(k >= 2)
        def _():
            for c, d in CD:
                pl.semaphore_wait(credit.at[c, d], 1)
        for c, d in CD:
            h(k, c, d).start()

    def give_credit(k, credit, ring):
        @pl.when(k + 2 < nch)
        def _():
            for c, d in CD:
                pl.semaphore_signal(
                    credit.at[c, d], inc=1, device_id={"tp": ring[c][1 - d]}, device_id_type=MESH
                )

    def ring_at(p, off):
        return lax.rem(p + off, SIDE)

    def piece(s, c, q):
        if c == 0:
            return lambda lo, n: cs[s, q, pl.ds(lo, n), :, pl.ds(0, L)]
        return lambda lo, n: cs[s, pl.ds(lo, n), q, :, pl.ds(L, L)]

    def grads_copy(k):
        s = lax.rem(k, 2)
        return pltpu.make_async_copy(
            dt.at[s], grads.at[:, pl.ds(pl.multiple_of(k * R, R), R)], dt_sem.at[s]
        )

    def stage_a(w, wdv, k):
        s = lax.rem(k, 2)
        for c in fetch(k):
            c.wait()

        @pl.when(k == 0)
        def _():
            weight_copies(w, wdv)[0].wait()

        depth = dyv.shape[1] // 4
        dh[...] = jnp.zeros_like(dh)

        @pl.loop(0, 4)
        def _(j):
            cols = pl.ds(pl.multiple_of(j * depth, depth), depth)
            dh[...] += lax.dot_general(wdv[:, cols], dyv[:, cols], NT, preferred_element_type=F32)

        @pl.when(k >= 2)
        def _():
            grads_copy(k - 2).wait()

        g = gv[...].astype(F32).T
        u = uv[...].astype(F32).T
        d = dh[...]
        sig = 1.0 / (1.0 + jnp.exp(-g))
        silu = g * sig
        dt[s, pl.ds(2 * f, f)] = (silu * u).astype(BF16)
        dt[s, pl.ds(f, f)] = (d * silu).astype(BF16)
        dt[s, pl.ds(0, f)] = (d * u * (sig + silu * (1.0 - sig))).astype(BF16)
        grads_copy(k).start()

        @pl.when(k + 1 < nch)
        def _():
            for c in fetch(k + 1):
                c.start()

    def rows_of(h, a):
        return pl.ds(pl.multiple_of(h * half + a * quarter, quarter), quarter)

    def stage_b(w, wdv, k):
        s = lax.rem(k, 2)

        @pl.when(k == 0)
        def _():
            for copy in weight_copies(w, wdv)[1:3]:
                copy.wait()

        @pl.when(k >= 2)
        def _():
            pl.semaphore_wait(cp, 1)

        @pl.loop(0, SIDE)
        def _(a):
            @pl.when(k >= 2)
            def _():
                pair_copy(k - 2, a).wait_send()

            t = jnp.dot(w[rows_of(1 - core, a)], dt[s, pl.ds(0, 2 * f)], preferred_element_type=F32)
            obuf[s, a] = t.astype(BF16).reshape(SIDE, sub, R)
            pair_copy(k, a).start()

    def stage_c(w, wdv, k):
        s = lax.rem(k, 2)

        @pl.when(k == 0)
        def _():
            for copy in weight_copies(w, wdv)[3:]:
                copy.wait()

        @pl.loop(0, SIDE)
        def _(a):
            t = jnp.dot(w[rows_of(core, a)], dt[s, pl.ds(0, 2 * f)], preferred_element_type=F32)
            pair_copy(k, a).wait_recv()
            cs[s, a] = t.reshape(SIDE, sub, R) + pbuf[s, a].astype(F32)

        @pl.when(k + 2 < nch)
        def _():
            pl.semaphore_signal(cp, inc=1, device_id={"tp": partner}, device_id_type=MESH)

    def stage_1a(k):
        s = lax.rem(k, 2)
        before_fill(k, h1a)
        for c in range(2):
            take = piece(s, c, ring_at(pos1[c], 2))
            for d in range(2):
                s1a[s, c, d] = take(2 * d, 2).astype(BF16)
        launch(k, h1a, c1a)

    def stage_1b(k):
        s = lax.rem(k, 2)
        before_fill(k, h1b)
        for c, d in CD:
            h1a(k, c, d).wait_recv()
            take = piece(s, c, ring_at(pos1[c], 1 if d == 0 else SIDE - 1))
            s1b[s, c, d, pl.ds(2 * d, 2)] = (take(2 * d, 2) + r1a[s, c, d].astype(F32)).astype(BF16)
            s1b[s, c, d, pl.ds(2 - 2 * d, 2)] = take(2 - 2 * d, 2).astype(BF16)
        launch(k, h1b, c1b)
        give_credit(k, c1a, ring1)

    def stage_1c(k):
        s = lax.rem(k, 2)
        for c in range(2):
            for d in range(2):
                h1b(k, c, d).wait_recv()
            p1[s, c] = piece(s, c, pos1[c])(0, SIDE) + r1b[s, c, 0].astype(F32) + r1b[s, c, 1].astype(F32)
        give_credit(k, c1b, ring1)

    def stage_2a(k):
        s = lax.rem(k, 2)
        before_fill(k, h2a)
        for c, d in CD:
            s2a[s, c, d] = p1[s, c, ring_at(pos2[c], 2), pl.ds(d * hs, hs)].astype(BF16)
        launch(k, h2a, c2a)

    def stage_2b(k):
        s = lax.rem(k, 2)
        before_fill(k, h2b)
        for c, d in CD:
            h2a(k, c, d).wait_recv()
            q = ring_at(pos2[c], 1 if d == 0 else SIDE - 1)
            same, other = pl.ds(d * hs, hs), pl.ds((1 - d) * hs, hs)
            s2b[s, c, d, same] = (p1[s, c, q, same] + r2a[s, c, d].astype(F32)).astype(BF16)
            s2b[s, c, d, other] = p1[s, c, q, other].astype(BF16)
        launch(k, h2b, c2b)
        give_credit(k, c2a, ring2)

    def stage_2c(k):
        s = lax.rem(k, 2)
        for c in range(2):
            for d in range(2):
                h2b(k, c, d).wait_recv()
            total = p1[s, c, pos2[c]] + r2b[s, c, 0].astype(F32) + r2b[s, c, 1].astype(F32)
            fin[k, c] = total.astype(BF16)
        give_credit(k, c2b, ring2)

    def own_copy(k, c):
        return pltpu.make_async_copy(fin.at[k, c], whole.at[k, core, c, pos1[c], pos2[c]], fin_sem.at[k, c])

    def spread(k, c, d, src, dst, ssem, rsem, ring):
        return remote(src, dst, ssem.at[k, c, d], rsem.at[k, c, d], ring[c][d])

    def came_from(p, d):
        return ring_at(p, SIDE - 1 if d == 0 else 1)

    def h3a(k, c, d):
        dst = whole.at[k, core, c, pos1[c], pos2[c]]
        return spread(k, c, d, fin.at[k, c], dst, ss3a, sr3a, ring2)

    def h3b(k, c, d):
        at3 = whole.at[k, core, c, pos1[c], came_from(pos2[c], d), pl.ds(d * hs, hs)]
        return spread(k, c, d, at3, at3, ss3b, sr3b, ring2)

    def h4a(k, c, d):
        at4 = whole.at[k, core, c, pos1[c]]
        return spread(k, c, d, at4, at4, ss4a, sr4a, ring1)

    def h4b(k, c, d):
        at4 = whole.at[k, core, c, came_from(pos1[c], d), pl.ds(2 * d, 2)]
        return spread(k, c, d, at4, at4, ss4b, sr4b, ring1)

    def h5(k, c):
        at5 = whole.at[k, core, c]
        return remote(at5, at5, ss5.at[k, c], sr5.at[k, c], partner)

    def stage_3a(k):
        for c in range(2):
            own_copy(k, c).start()
        for c, d in CD:
            h3a(k, c, d).start()

    def stage_3b(k):
        for c, d in CD:
            h3a(k, c, d).wait_recv()
            h3b(k, c, d).start()

    def stage_4a(k):
        for c in range(2):
            own_copy(k, c).wait()
            for d in range(2):
                h3b(k, c, d).wait_recv()
            for d in range(2):
                h4a(k, c, d).start()

    def stage_4b(k):
        for c, d in CD:
            h4a(k, c, d).wait_recv()
            h4b(k, c, d).start()

    def stage_5(k):
        for c in range(2):
            for d in range(2):
                h4b(k, c, d).wait_recv()
            h5(k, c).start()

    def run(stage, k):
        @pl.when((k >= 0) & (k < nch))
        def _():
            stage(k)

    def terms(w, wdv):
        copies = weight_copies(w, wdv)
        first = fetch(0)
        first[0].start()
        copies[0].start()
        first[1].start()
        first[2].start()
        for copy in copies[1:]:
            copy.start()

        barrier = pltpu.get_barrier_semaphore()
        for peer in (partner, *xn, *yn):
            pl.semaphore_signal(barrier, inc=1, device_id={"tp": peer}, device_id_type=MESH)
        pl.semaphore_wait(barrier, 5)

        @pl.loop(0, nch)
        def _(i):
            stage_a(w, wdv, i)
            run(stage_2b, i - 3)
            stage_b(w, wdv, i)
            run(stage_1c, i - 2)
            run(stage_2a, i - 2)
            run(stage_1b, i - 1)
            stage_c(w, wdv, i)
            stage_1a(i)
            run(stage_2c, i - 3)
            run(stage_3a, i - O3A)
            run(stage_3b, i - O3B)
            run(stage_4a, i - O4A)
            run(stage_4b, i - O4B)
            run(stage_5, i - O5)

    pl.run_scoped(terms, pltpu.VMEM((2 * half, 2 * f), BF16), pltpu.VMEM((f, 2 * half), BF16))

    for k in (nch - 2, nch - 1):
        grads_copy(k).wait()

    blocks = 2 * half // N
    tail = nch + O5
    per_step = -(-blocks // (tail - nch))

    def weights(gr, xv, dv, gst, dst):
        load = pltpu.make_async_copy(grads, gr, g_sem)

        def cols(j):
            return pl.ds(pl.multiple_of(j * N, N), N)

        def ins(j):
            s = lax.rem(j, 2)
            return [
                pltpu.make_async_copy(x_in.at[:, cols(j)], xv.at[s], x_sem.at[s, 0]),
                pltpu.make_async_copy(dy.at[:, cols(j)], dv.at[s], x_sem.at[s, 1]),
            ]

        def results(j):
            s = lax.rem(j, 2)
            return [
                pltpu.make_async_copy(gst.at[s, 0], dwg.at[cols(j)], o_sem.at[s, 0]),
                pltpu.make_async_copy(gst.at[s, 1], dwu.at[cols(j)], o_sem.at[s, 1]),
                pltpu.make_async_copy(dst.at[s], dwd.at[:, cols(j)], o_sem.at[s, 2]),
            ]

        def unit(j):
            s = lax.rem(j, 2)

            @pl.when(j == 0)
            def _():
                load.wait()

            for copy in ins(j):
                copy.wait()

            @pl.when(j >= 2)
            def _():
                for copy in results(j - 2):
                    copy.wait()

            for m in range(2):
                t = jnp.dot(gr[pl.ds(m * f, f)], xv[s], preferred_element_type=F32)
                gst[s, m] = t.T.astype(BF16)
            dst[s] = jnp.dot(gr[pl.ds(2 * f, f)], dv[s], preferred_element_type=F32).astype(BF16)
            for copy in results(j):
                copy.start()

            @pl.when(j + 2 < blocks)
            def _():
                for copy in ins(j + 2):
                    copy.start()

        def units(lo, hi):
            @pl.loop(lo, hi)
            def _(j):
                @pl.when(j < blocks)
                def _():
                    unit(j)

        load.start()
        for j in (0, 1):
            for copy in ins(j):
                copy.start()

        split = per_step // 2

        @pl.loop(nch, tail)
        def _(i):
            j = (i - nch) * per_step
            run(stage_2b, i - 3)
            run(stage_1c, i - 2)
            run(stage_2a, i - 2)
            run(stage_1b, i - 1)
            units(j, j + split)
            run(stage_2c, i - 3)
            run(stage_3a, i - O3A)
            run(stage_3b, i - O3B)
            units(j + split, j + per_step)
            run(stage_4a, i - O4A)
            run(stage_4b, i - O4B)
            run(stage_5, i - O5)

        for j in (blocks - 2, blocks - 1):
            for copy in results(j):
                copy.wait()

    pl.run_scoped(
        weights,
        pltpu.VMEM((3 * f, nch * R), BF16),
        pltpu.VMEM((2, nch * R, N), BF16),
        pltpu.VMEM((2, nch * R, N), BF16),
        pltpu.VMEM((2, 2, N, f), BF16),
        pltpu.VMEM((2, f, N), BF16),
    )

    for k in (nch - 2, nch - 1):
        for a in range(SIDE):
            pair_copy(k, a).wait_send()
        for h in (h1a, h1b, h2a, h2b):
            for c, d in CD:
                h(k, c, d).wait_send()

    @pl.loop(0, nch)
    def _(k):
        for h in (h3a, h3b, h4a, h4b):
            for c, d in CD:
                h(k, c, d).wait_send()
        for c in range(2):
            h5(k, c).wait()


def block_call(x, dy, gate, up, wg, wu, wd):
    rows, d = dy.shape
    f = wg.shape[1]
    nch = rows // R
    sub = d // (2 * SIDE * SIDE)
    ANY = pl.BlockSpec(memory_space=pl.ANY)
    dma = pltpu.SemaphoreType.DMA
    return pl.pallas_call(
        functools.partial(block_kernel, nch),
        out_shape=[
            jax.ShapeDtypeStruct((3 * f, rows), BF16),
            jax.ShapeDtypeStruct((nch, 2, 2, SIDE, SIDE, sub, L), BF16),
            jax.ShapeDtypeStruct((d, f), BF16),
            jax.ShapeDtypeStruct((d, f), BF16),
            jax.ShapeDtypeStruct((f, d), BF16),
        ],
        in_specs=[ANY] * 7,
        out_specs=[ANY] * 5,
        scratch_shapes=[
            pltpu.VMEM((R, d), BF16),
            pltpu.VMEM((R, f), BF16),
            pltpu.VMEM((R, f), BF16),
            pltpu.VMEM((f, R), F32),
            pltpu.VMEM((2, 3 * f, R), BF16),
            pltpu.VMEM((2, SIDE, SIDE, sub, R), BF16),
            pltpu.VMEM((2, SIDE, SIDE, sub, R), BF16),
            pltpu.VMEM((2, SIDE, SIDE, sub, R), F32),
            pltpu.VMEM((2, 2, 2, 2, sub, L), BF16),
            pltpu.VMEM((2, 2, 2, 2, sub, L), BF16),
            pltpu.VMEM((2, 2, 2, SIDE, sub, L), BF16),
            pltpu.VMEM((2, 2, 2, SIDE, sub, L), BF16),
            pltpu.VMEM((2, 2, SIDE, sub, L), F32),
            pltpu.VMEM((2, 2, 2, sub // 2, L), BF16),
            pltpu.VMEM((2, 2, 2, sub // 2, L), BF16),
            pltpu.VMEM((2, 2, 2, sub, L), BF16),
            pltpu.VMEM((2, 2, 2, sub, L), BF16),
            pltpu.VMEM((nch, 2, sub, L), BF16),
            dma((3,)),
            dma((5,)),
            dma((2,)),
            dma((nch, 2)),
            dma((2, SIDE)),
            dma((2, SIDE)),
        ]
        + [dma((2, 2, 2))] * 8
        + [dma((nch, 2, 2))] * 8
        + [dma((nch, 2))] * 2
        + [dma, dma((2, 2)), dma((2, 3))]
        + [pltpu.SemaphoreType.REGULAR]
        + [pltpu.SemaphoreType.REGULAR((2, 2))] * 4,
        compiler_params=pltpu.CompilerParams(
            collective_id=0, has_side_effects=True, vmem_limit_bytes=VMEM_LIMIT
        ),
        cost_estimate=pl.CostEstimate(
            flops=12 * rows * d * f, bytes_accessed=8 * rows * d + 12 * d * f, transcendentals=rows * f
        ),
        name="mlp_backward",
    )(x, dy, gate, up, wg, wu, wd)


def place_kernel(g, wg_in, wu_in, wd_in, out, wg_out, wu_out, wd_out):
    @pl.when(pl.program_id(1) == 0)
    def _():
        wg_out[...] = wg_in[...]
        wu_out[...] = wu_in[...]
        wd_out[...] = wd_in[...]

    for c in range(2):
        for a in range(SIDE):
            pieces = [g[0, 0, c, a, b] if c == 0 else g[0, 0, c, b, a] for b in range(SIDE)]
            stacked = jnp.concatenate(pieces, axis=0)
            n = stacked.shape[0]
            out[0, pl.ds(c * L, L), pl.ds(a * n, n)] = stacked.T


def place_call(whole, dwg, dwu, dwd):
    nch, _, _, _, _, sub, _ = whole.shape
    half = sub * SIDE * SIDE
    d, f = dwg.shape
    n = d // nch
    tall = pl.BlockSpec((n, f), lambda k, c: (k, 0))
    wide = pl.BlockSpec((f, n), lambda k, c: (0, k))
    return pl.pallas_call(
        place_kernel,
        grid=(nch, 2),
        out_shape=[
            jax.ShapeDtypeStruct((nch, R, d), BF16),
            jax.ShapeDtypeStruct((d, f), BF16),
            jax.ShapeDtypeStruct((d, f), BF16),
            jax.ShapeDtypeStruct((f, d), BF16),
        ],
        in_specs=[
            pl.BlockSpec((1, 1, 2, SIDE, SIDE, sub, L), lambda k, c: (k, c, 0, 0, 0, 0, 0)),
            tall,
            tall,
            wide,
        ],
        out_specs=[pl.BlockSpec((1, R, half), lambda k, c: (k, 0, c)), tall, tall, wide],
        compiler_params=pltpu.CompilerParams(vmem_limit_bytes=60 * 2**20),
        cost_estimate=pl.CostEstimate(
            flops=nch * R * half * 64, bytes_accessed=8 * nch * R * half + 12 * d * f, transcendentals=0
        ),
        name="place",
    )(whole, dwg, dwu, dwd)


def solution(mesh):
    def step(x, dy, gate, up, w_gate, w_up, w_down):
        _, whole, *grads = block_call(x, dy, gate, up, w_gate, w_up, w_down)
        dx, *grads = place_call(whole, *grads)
        return dx.reshape(x.shape), *grads

    tokens, columns, rows = P("dp", None), P(None, "tp"), P("tp", None)
    return jax.shard_map(
        step,
        mesh=mesh,
        in_specs=(tokens, tokens, P("dp", "tp"), P("dp", "tp"), columns, columns, rows),
        out_specs=(tokens, P("dp", "tp"), P("dp", "tp"), P(("dp", "tp"), None)),
        check_vma=False,
    )
```

```python
import functools

import jax
import jax.numpy as jnp
from jax import lax
from jax.experimental import pallas as pl
from jax.experimental.pallas import tpu as pltpu
from jax.sharding import PartitionSpec as P

MESH = pl.DeviceIdType.MESH
BF16, F32 = jnp.bfloat16, jnp.float32
R = 256
L = 128
SIDE = 4
N = 256
O3A, O3B, O4A, O4B, O5 = 6, 7, 8, 9, 10
NT = (((1,), (1,)), ((), ()))
VMEM_LIMIT = 66_900_000


def block_kernel(
    nch, x_in, dy, gate, up, wg, wu, wd, grads, whole, dwg, dwu, dwd,
    dyv, gv, uv, dh, dt, obuf, pbuf, cs, s1a, r1a, s1b, r1b, p1, s2a, r2a, s2b, r2b, fin,
    in_sem, w_sem, dt_sem, fin_sem, ps, pr, ss1a, sr1a, ss1b, sr1b, ss2a, sr2a, ss2b, sr2b,
    ss3a, sr3a, ss3b, sr3b, ss4a, sr4a, ss4b, sr4b, ss5, sr5, g_sem, x_sem, o_sem,
    cp, c1a, c1b, c2a, c2b,
):
    f = wg.shape[1]
    half = wg.shape[0] // 2
    quarter = half // SIDE
    sub = quarter // SIDE
    hs = sub // 2

    me = lax.axis_index("tp")
    core = lax.rem(me, 2)
    y = lax.rem(me // 2, SIDE)
    x = me // (2 * SIDE)

    def at(i, j, c):
        return (lax.rem(i + SIDE, SIDE) * SIDE + lax.rem(j + SIDE, SIDE)) * 2 + c

    partner = at(x, y, 1 - core)
    xn = (at(x + 1, y, core), at(x - 1, y, core))
    yn = (at(x, y + 1, core), at(x, y - 1, core))
    ring1, pos1 = (xn, yn), (x, y)
    ring2, pos2 = (yn, xn), (y, x)

    def fetch(k):
        rows = pl.ds(pl.multiple_of(k * R, R), R)
        return [
            pltpu.make_async_copy(dy.at[rows], dyv, in_sem.at[0]),
            pltpu.make_async_copy(gate.at[rows], gv, in_sem.at[1]),
            pltpu.make_async_copy(up.at[rows], uv, in_sem.at[2]),
        ]

    def weight_copies(w, wdv):
        copies = [pltpu.make_async_copy(wd, wdv, w_sem.at[0])]
        for i, h in enumerate((1 - core, core)):
            rows = pl.ds(pl.multiple_of(h * half, half), half)
            for m, source in enumerate((wg, wu)):
                copies.append(
                    pltpu.make_async_copy(
                        source.at[rows], w.at[rows, pl.ds(m * f, f)], w_sem.at[1 + 2 * i + m]
                    )
                )
        return copies

    def remote(src, dst, ssem, rsem, dev):
        return pltpu.make_async_remote_copy(
            src_ref=src, dst_ref=dst, send_sem=ssem, recv_sem=rsem,
            device_id={"tp": dev}, device_id_type=MESH,
        )

    def pair_copy(k, a):
        s = lax.rem(k, 2)
        return remote(obuf.at[s, a], pbuf.at[s, a], ps.at[s, a], pr.at[s, a], partner)

    def hop(k, c, d, src, dst, ssem, rsem, ring):
        s = lax.rem(k, 2)
        return remote(src.at[s, c, d], dst.at[s, c, d], ssem.at[s, c, d], rsem.at[s, c, d], ring[c][d])

    h1a = lambda k, c, d: hop(k, c, d, s1a, r1a, ss1a, sr1a, ring1)
    h1b = lambda k, c, d: hop(k, c, d, s1b, r1b, ss1b, sr1b, ring1)
    h2a = lambda k, c, d: hop(k, c, d, s2a, r2a, ss2a, sr2a, ring2)
    h2b = lambda k, c, d: hop(k, c, d, s2b, r2b, ss2b, sr2b, ring2)
    CD = [(c, d) for c in range(2) for d in range(2)]

    def before_fill(k, h):
        @pl.when(k >= 2)
        def _():
            for c, d in CD:
                h(k - 2, c, d).wait_send()

    def launch(k, h, credit):
        @pl.when(k >= 2)
        def _():
            for c, d in CD:
                pl.semaphore_wait(credit.at[c, d], 1)
        for c, d in CD:
            h(k, c, d).start()

    def give_credit(k, credit, ring):
        @pl.when(k + 2 < nch)
        def _():
            for c, d in CD:
                pl.semaphore_signal(
                    credit.at[c, d], inc=1, device_id={"tp": ring[c][1 - d]}, device_id_type=MESH
                )

    def ring_at(p, off):
        return lax.rem(p + off, SIDE)

    def piece(s, c, q):
        if c == 0:
            return lambda lo, n: cs[s, q, pl.ds(lo, n), :, pl.ds(0, L)]
        return lambda lo, n: cs[s, pl.ds(lo, n), q, :, pl.ds(L, L)]

    def grads_copy(k):
        s = lax.rem(k, 2)
        return pltpu.make_async_copy(
            dt.at[s], grads.at[:, pl.ds(pl.multiple_of(k * R, R), R)], dt_sem.at[s]
        )

    def stage_a(w, wdv, k):
        s = lax.rem(k, 2)
        for c in fetch(k):
            c.wait()

        @pl.when(k == 0)
        def _():
            weight_copies(w, wdv)[0].wait()

        depth = dyv.shape[1] // 4
        dh[...] = jnp.zeros_like(dh)

        @pl.loop(0, 4)
        def _(j):
            cols = pl.ds(pl.multiple_of(j * depth, depth), depth)
            dh[...] += lax.dot_general(wdv[:, cols], dyv[:, cols], NT, preferred_element_type=F32)

        @pl.when(k >= 2)
        def _():
            grads_copy(k - 2).wait()

        g = gv[...].astype(F32).T
        u = uv[...].astype(F32).T
        d = dh[...]
        sig = 1.0 / (1.0 + jnp.exp(-g))
        silu = g * sig
        dt[s, pl.ds(2 * f, f)] = (silu * u).astype(BF16)
        dt[s, pl.ds(f, f)] = (d * silu).astype(BF16)
        dt[s, pl.ds(0, f)] = (d * u * (sig + silu * (1.0 - sig))).astype(BF16)
        grads_copy(k).start()

        @pl.when(k + 1 < nch)
        def _():
            for c in fetch(k + 1):
                c.start()

    def rows_of(h, a):
        return pl.ds(pl.multiple_of(h * half + a * quarter, quarter), quarter)

    def stage_b(w, wdv, k):
        s = lax.rem(k, 2)

        @pl.when(k == 0)
        def _():
            for copy in weight_copies(w, wdv)[1:3]:
                copy.wait()

        @pl.when(k >= 2)
        def _():
            pl.semaphore_wait(cp, 1)

        @pl.loop(0, SIDE)
        def _(a):
            @pl.when(k >= 2)
            def _():
                pair_copy(k - 2, a).wait_send()

            t = jnp.dot(w[rows_of(1 - core, a)], dt[s, pl.ds(0, 2 * f)], preferred_element_type=F32)
            obuf[s, a] = t.astype(BF16).reshape(SIDE, sub, R)
            pair_copy(k, a).start()

    def stage_c(w, wdv, k):
        s = lax.rem(k, 2)

        @pl.when(k == 0)
        def _():
            for copy in weight_copies(w, wdv)[3:]:
                copy.wait()

        @pl.loop(0, SIDE)
        def _(a):
            t = jnp.dot(w[rows_of(core, a)], dt[s, pl.ds(0, 2 * f)], preferred_element_type=F32)
            pair_copy(k, a).wait_recv()
            cs[s, a] = t.reshape(SIDE, sub, R) + pbuf[s, a].astype(F32)

        @pl.when(k + 2 < nch)
        def _():
            pl.semaphore_signal(cp, inc=1, device_id={"tp": partner}, device_id_type=MESH)

    def stage_1a(k):
        s = lax.rem(k, 2)
        before_fill(k, h1a)
        for c in range(2):
            take = piece(s, c, ring_at(pos1[c], 2))
            for d in range(2):
                s1a[s, c, d] = take(2 * d, 2).astype(BF16)
        launch(k, h1a, c1a)

    def stage_1b(k):
        s = lax.rem(k, 2)
        before_fill(k, h1b)
        for c, d in CD:
            h1a(k, c, d).wait_recv()
            take = piece(s, c, ring_at(pos1[c], 1 if d == 0 else SIDE - 1))
            s1b[s, c, d, pl.ds(2 * d, 2)] = (take(2 * d, 2) + r1a[s, c, d].astype(F32)).astype(BF16)
            s1b[s, c, d, pl.ds(2 - 2 * d, 2)] = take(2 - 2 * d, 2).astype(BF16)
        launch(k, h1b, c1b)
        give_credit(k, c1a, ring1)

    def stage_1c(k):
        s = lax.rem(k, 2)
        for c in range(2):
            for d in range(2):
                h1b(k, c, d).wait_recv()
            p1[s, c] = piece(s, c, pos1[c])(0, SIDE) + r1b[s, c, 0].astype(F32) + r1b[s, c, 1].astype(F32)
        give_credit(k, c1b, ring1)

    def stage_2a(k):
        s = lax.rem(k, 2)
        before_fill(k, h2a)
        for c, d in CD:
            s2a[s, c, d] = p1[s, c, ring_at(pos2[c], 2), pl.ds(d * hs, hs)].astype(BF16)
        launch(k, h2a, c2a)

    def stage_2b(k):
        s = lax.rem(k, 2)
        before_fill(k, h2b)
        for c, d in CD:
            h2a(k, c, d).wait_recv()
            q = ring_at(pos2[c], 1 if d == 0 else SIDE - 1)
            same, other = pl.ds(d * hs, hs), pl.ds((1 - d) * hs, hs)
            s2b[s, c, d, same] = (p1[s, c, q, same] + r2a[s, c, d].astype(F32)).astype(BF16)
            s2b[s, c, d, other] = p1[s, c, q, other].astype(BF16)
        launch(k, h2b, c2b)
        give_credit(k, c2a, ring2)

    def stage_2c(k):
        s = lax.rem(k, 2)
        for c in range(2):
            for d in range(2):
                h2b(k, c, d).wait_recv()
            total = p1[s, c, pos2[c]] + r2b[s, c, 0].astype(F32) + r2b[s, c, 1].astype(F32)
            fin[k, c] = total.astype(BF16)
        give_credit(k, c2b, ring2)

    def own_copy(k, c):
        return pltpu.make_async_copy(fin.at[k, c], whole.at[k, core, c, pos1[c], pos2[c]], fin_sem.at[k, c])

    def spread(k, c, d, src, dst, ssem, rsem, ring):
        return remote(src, dst, ssem.at[k, c, d], rsem.at[k, c, d], ring[c][d])

    def came_from(p, d):
        return ring_at(p, SIDE - 1 if d == 0 else 1)

    def h3a(k, c, d):
        dst = whole.at[k, core, c, pos1[c], pos2[c]]
        return spread(k, c, d, fin.at[k, c], dst, ss3a, sr3a, ring2)

    def h3b(k, c, d):
        at3 = whole.at[k, core, c, pos1[c], came_from(pos2[c], d), pl.ds(d * hs, hs)]
        return spread(k, c, d, at3, at3, ss3b, sr3b, ring2)

    def h4a(k, c, d):
        at4 = whole.at[k, core, c, pos1[c]]
        return spread(k, c, d, at4, at4, ss4a, sr4a, ring1)

    def h4b(k, c, d):
        at4 = whole.at[k, core, c, came_from(pos1[c], d), pl.ds(2 * d, 2)]
        return spread(k, c, d, at4, at4, ss4b, sr4b, ring1)

    def h5(k, c, off):
        at5 = whole.at[k, core, c, ring_at(pos1[c], off)]
        return remote(at5, at5, ss5.at[k, c, off], sr5.at[k, c, off], partner)

    def stage_3a(k):
        for c in range(2):
            own_copy(k, c).start()
        for c, d in CD:
            h3a(k, c, d).start()

    def stage_3b(k):
        for c, d in CD:
            h3a(k, c, d).wait_recv()
            h3b(k, c, d).start()

    def stage_4a(k):
        for c in range(2):
            own_copy(k, c).wait()
            for d in range(2):
                h3b(k, c, d).wait_recv()
            for d in range(2):
                h4a(k, c, d).start()
            h5(k, c, 0).start()

    def stage_4b(k):
        for c, d in CD:
            h4a(k, c, d).wait_recv()
            h4b(k, c, d).start()
            h5(k, c, SIDE - 1 if d == 0 else 1).start()

    def stage_5(k):
        for c in range(2):
            for d in range(2):
                h4b(k, c, d).wait_recv()
            h5(k, c, 2).start()

    def run(stage, k):
        @pl.when((k >= 0) & (k < nch))
        def _():
            stage(k)

    def terms(w, wdv):
        copies = weight_copies(w, wdv)
        first = fetch(0)
        first[0].start()
        copies[0].start()
        first[1].start()
        first[2].start()
        for copy in copies[1:]:
            copy.start()

        barrier = pltpu.get_barrier_semaphore()
        for peer in (partner, *xn, *yn):
            pl.semaphore_signal(barrier, inc=1, device_id={"tp": peer}, device_id_type=MESH)
        pl.semaphore_wait(barrier, 5)

        @pl.loop(0, nch)
        def _(i):
            stage_a(w, wdv, i)
            run(stage_2b, i - 3)
            stage_b(w, wdv, i)
            run(stage_1c, i - 2)
            run(stage_2a, i - 2)
            run(stage_1b, i - 1)
            stage_c(w, wdv, i)
            stage_1a(i)
            run(stage_2c, i - 3)
            run(stage_3a, i - O3A)
            run(stage_3b, i - O3B)
            run(stage_4a, i - O4A)
            run(stage_4b, i - O4B)
            run(stage_5, i - O5)

    pl.run_scoped(terms, pltpu.VMEM((2 * half, 2 * f), BF16), pltpu.VMEM((f, 2 * half), BF16))

    for k in (nch - 2, nch - 1):
        grads_copy(k).wait()

    blocks = 2 * half // N
    tail = nch + O5
    per_step = -(-blocks // (tail - nch))

    def weights(gr, xv, dv, gst, dst):
        load = pltpu.make_async_copy(grads, gr, g_sem)

        def cols(j):
            return pl.ds(pl.multiple_of(j * N, N), N)

        def ins(j):
            s = lax.rem(j, 2)
            return [
                pltpu.make_async_copy(x_in.at[:, cols(j)], xv.at[s], x_sem.at[s, 0]),
                pltpu.make_async_copy(dy.at[:, cols(j)], dv.at[s], x_sem.at[s, 1]),
            ]

        def results(j):
            s = lax.rem(j, 2)
            return [
                pltpu.make_async_copy(gst.at[s, 0], dwg.at[cols(j)], o_sem.at[s, 0]),
                pltpu.make_async_copy(gst.at[s, 1], dwu.at[cols(j)], o_sem.at[s, 1]),
                pltpu.make_async_copy(dst.at[s], dwd.at[:, cols(j)], o_sem.at[s, 2]),
            ]

        def unit(j):
            s = lax.rem(j, 2)

            @pl.when(j == 0)
            def _():
                load.wait()

            for copy in ins(j):
                copy.wait()

            @pl.when(j >= 2)
            def _():
                for copy in results(j - 2):
                    copy.wait()

            for m in range(2):
                t = jnp.dot(gr[pl.ds(m * f, f)], xv[s], preferred_element_type=F32)
                gst[s, m] = t.T.astype(BF16)
            dst[s] = jnp.dot(gr[pl.ds(2 * f, f)], dv[s], preferred_element_type=F32).astype(BF16)
            for copy in results(j):
                copy.start()

            @pl.when(j + 2 < blocks)
            def _():
                for copy in ins(j + 2):
                    copy.start()

        def units(lo, hi):
            @pl.loop(lo, hi)
            def _(j):
                @pl.when(j < blocks)
                def _():
                    unit(j)

        load.start()
        for j in (0, 1):
            for copy in ins(j):
                copy.start()

        split = per_step // 2

        @pl.loop(nch, tail)
        def _(i):
            j = (i - nch) * per_step
            run(stage_2b, i - 3)
            run(stage_1c, i - 2)
            run(stage_2a, i - 2)
            run(stage_1b, i - 1)
            units(j, j + split)
            run(stage_2c, i - 3)
            run(stage_3a, i - O3A)
            run(stage_3b, i - O3B)
            units(j + split, j + per_step)
            run(stage_4a, i - O4A)
            run(stage_4b, i - O4B)
            run(stage_5, i - O5)

        for j in (blocks - 2, blocks - 1):
            for copy in results(j):
                copy.wait()

    pl.run_scoped(
        weights,
        pltpu.VMEM((3 * f, nch * R), BF16),
        pltpu.VMEM((2, nch * R, N), BF16),
        pltpu.VMEM((2, nch * R, N), BF16),
        pltpu.VMEM((2, 2, N, f), BF16),
        pltpu.VMEM((2, f, N), BF16),
    )

    for k in (nch - 2, nch - 1):
        for a in range(SIDE):
            pair_copy(k, a).wait_send()
        for h in (h1a, h1b, h2a, h2b):
            for c, d in CD:
                h(k, c, d).wait_send()

    @pl.loop(0, nch)
    def _(k):
        for h in (h3a, h3b, h4a, h4b):
            for c, d in CD:
                h(k, c, d).wait_send()
        for c in range(2):
            for off in range(SIDE):
                h5(k, c, off).wait()


def block_call(x, dy, gate, up, wg, wu, wd):
    rows, d = dy.shape
    f = wg.shape[1]
    nch = rows // R
    sub = d // (2 * SIDE * SIDE)
    ANY = pl.BlockSpec(memory_space=pl.ANY)
    dma = pltpu.SemaphoreType.DMA
    return pl.pallas_call(
        functools.partial(block_kernel, nch),
        out_shape=[
            jax.ShapeDtypeStruct((3 * f, rows), BF16),
            jax.ShapeDtypeStruct((nch, 2, 2, SIDE, SIDE, sub, L), BF16),
            jax.ShapeDtypeStruct((d, f), BF16),
            jax.ShapeDtypeStruct((d, f), BF16),
            jax.ShapeDtypeStruct((f, d), BF16),
        ],
        in_specs=[ANY] * 7,
        out_specs=[ANY] * 5,
        scratch_shapes=[
            pltpu.VMEM((R, d), BF16),
            pltpu.VMEM((R, f), BF16),
            pltpu.VMEM((R, f), BF16),
            pltpu.VMEM((f, R), F32),
            pltpu.VMEM((2, 3 * f, R), BF16),
            pltpu.VMEM((2, SIDE, SIDE, sub, R), BF16),
            pltpu.VMEM((2, SIDE, SIDE, sub, R), BF16),
            pltpu.VMEM((2, SIDE, SIDE, sub, R), F32),
            pltpu.VMEM((2, 2, 2, 2, sub, L), BF16),
            pltpu.VMEM((2, 2, 2, 2, sub, L), BF16),
            pltpu.VMEM((2, 2, 2, SIDE, sub, L), BF16),
            pltpu.VMEM((2, 2, 2, SIDE, sub, L), BF16),
            pltpu.VMEM((2, 2, SIDE, sub, L), F32),
            pltpu.VMEM((2, 2, 2, sub // 2, L), BF16),
            pltpu.VMEM((2, 2, 2, sub // 2, L), BF16),
            pltpu.VMEM((2, 2, 2, sub, L), BF16),
            pltpu.VMEM((2, 2, 2, sub, L), BF16),
            pltpu.VMEM((nch, 2, sub, L), BF16),
            dma((3,)),
            dma((5,)),
            dma((2,)),
            dma((nch, 2)),
            dma((2, SIDE)),
            dma((2, SIDE)),
        ]
        + [dma((2, 2, 2))] * 8
        + [dma((nch, 2, 2))] * 8
        + [dma((nch, 2, SIDE))] * 2
        + [dma, dma((2, 2)), dma((2, 3))]
        + [pltpu.SemaphoreType.REGULAR]
        + [pltpu.SemaphoreType.REGULAR((2, 2))] * 4,
        compiler_params=pltpu.CompilerParams(
            collective_id=0, has_side_effects=True, vmem_limit_bytes=VMEM_LIMIT
        ),
        cost_estimate=pl.CostEstimate(
            flops=12 * rows * d * f, bytes_accessed=8 * rows * d + 12 * d * f, transcendentals=rows * f
        ),
        name="mlp_backward",
    )(x, dy, gate, up, wg, wu, wd)


def place_kernel(g, wg_in, wu_in, wd_in, out, wg_out, wu_out, wd_out):
    wg_out[...] = wg_in[...]
    wu_out[...] = wu_in[...]
    wd_out[...] = wd_in[...]

    for core in range(2):
        for c in range(2):
            for a in range(SIDE):
                pieces = [g[0, core, c, a, b] if c == 0 else g[0, core, c, b, a] for b in range(SIDE)]
                stacked = jnp.concatenate(pieces, axis=0)
                n = stacked.shape[0]
                out[0, pl.ds(c * L, L), pl.ds((core * SIDE + a) * n, n)] = stacked.T


def place_call(whole, dwg, dwu, dwd):
    nch, _, _, _, _, sub, _ = whole.shape
    d, f = dwg.shape
    n = d // nch
    tall = pl.BlockSpec((n, f), lambda k: (k, 0))
    wide = pl.BlockSpec((f, n), lambda k: (0, k))
    return pl.pallas_call(
        place_kernel,
        grid=(nch,),
        out_shape=[
            jax.ShapeDtypeStruct((nch, R, d), BF16),
            jax.ShapeDtypeStruct((d, f), BF16),
            jax.ShapeDtypeStruct((d, f), BF16),
            jax.ShapeDtypeStruct((f, d), BF16),
        ],
        in_specs=[
            pl.BlockSpec((1, 2, 2, SIDE, SIDE, sub, L), lambda k: (k, 0, 0, 0, 0, 0, 0)),
            tall,
            tall,
            wide,
        ],
        out_specs=[pl.BlockSpec((1, R, d), lambda k: (k, 0, 0)), tall, tall, wide],
        compiler_params=pltpu.CompilerParams(vmem_limit_bytes=60 * 2**20),
        cost_estimate=pl.CostEstimate(
            flops=nch * R * d * 32, bytes_accessed=4 * nch * R * d + 12 * d * f, transcendentals=0
        ),
        name="place",
    )(whole, dwg, dwu, dwd)


def solution(mesh):
    def step(x, dy, gate, up, w_gate, w_up, w_down):
        _, whole, *grads = block_call(x, dy, gate, up, w_gate, w_up, w_down)
        dx, *grads = place_call(whole, *grads)
        return dx.reshape(x.shape), *grads

    tokens, columns, rows = P("dp", None), P(None, "tp"), P("tp", None)
    return jax.shard_map(
        step,
        mesh=mesh,
        in_specs=(tokens, tokens, P("dp", "tp"), P("dp", "tp"), columns, columns, rows),
        out_specs=(tokens, P("dp", "tp"), P("dp", "tp"), P(("dp", "tp"), None)),
        check_vma=False,
    )
```
